128 devices in a mesh: shard: 16 (over x_hi, z, core), rep: 8 (over x_lo, y).
Axes of the slice: x: 4 (x_hi: 2, x_lo: 2; x = x_hi * 2 + x_lo), y: 4, z: 4, core: 2. Of those that a mesh axis runs over, the one named last changes fastest.
Arguments:
- tokens: bfloat16 [49152, 5120], P(('shard', 'rep')), may hold values from -700 to 700
- norm_gain: float32 [5120], replicated, may hold values from 0.1 to 1.9
- key_bias: float32 [1024], replicated, may hold values from -4 to 4
- key_weight: bfloat16 [8192, 1024], P('shard'), may hold values from -0.078125 to 0.078125
- cotangent: bfloat16 [49152, 1024], P(('shard', 'rep')), may hold values from -40 to 40
- block_slot: int32 [40], replicated, may hold values from 0 to 63, as said below
Outputs:
- projected: bfloat16 [49152, 1024], P(('shard', 'rep'))
- token_grad: bfloat16 [49152, 5120], P(('shard', 'rep'))
- weight_grad: float32 [8192, 1024], P('shard')
- gain_grad: float32 [5120], replicated
- bias_grad: float32 [1024], replicated
The draws below stay inside these ranges and needn't reach their ends.
Inputs may be any that keep to these rules, and one draw needn't show every extreme that they name: Entries are distinct; block b lies on the device of shard with index block_slot[b] // 4, at its local slot block_slot[b] % 4; in every draw some device holds 4 blocks.
All inputs are finite; a program needn't handle non-finite values.
Results may differ from the reference program's by a relative error of at most 0.013.
Values may be sent and summed in bfloat16 or wider, within the bound.
No kernel may reach another device: no remote copies, remote signals or barrier semaphores. Data moves between devices by JAX's collectives and lax.ppermute only.
A program may use at most 128 MiB of HBM per device.

```python
import math
import jax
import jax.numpy as jnp
from jax import lax

D = 5120
KVW = 1024
BLK = 128
TOK_DEV = 384
NBLK = 40
CAP = 4
SLOTS = 64
ALL_TOK = 49152
N_SHARD = 16


def draw_tokens(key, part):
    keys = jax.random.split(key, 3)
    row_scale = jnp.exp(jax.random.uniform(keys[0], (ALL_TOK, 1), minval=0.0, maxval=math.log(10.0)))
    col_scale = jnp.exp(jax.random.uniform(keys[1], (1, D), minval=0.0, maxval=math.log(10.0)))
    base = jnp.clip(jax.random.normal(keys[2], (ALL_TOK, D)), -6.0, 6.0)
    return (base * row_scale * col_scale).astype(jnp.bfloat16)


def draw_cotangent(key, part):
    keys = jax.random.split(key, 1)
    position = jnp.arange(ALL_TOK, dtype=jnp.float32)[:, None] / max(ALL_TOK - 1, 1)
    rising = 1.0 + 2.0 * position
    values = jnp.clip(jax.random.normal(keys[0], (ALL_TOK, KVW)), -6.0, 6.0) * rising
    return values.astype(jnp.bfloat16)


def draw_block_slot(key, part):
    keys = jax.random.split(key, 3)
    full_owner = jax.random.randint(keys[0], (), 0, N_SHARD)
    slot_ids = jnp.arange(SLOTS, dtype=jnp.int32)
    order_slots = jax.random.permutation(keys[1], SLOTS).astype(jnp.int32)
    scores = jnp.where(slot_ids // CAP == full_owner, 0, 1 + order_slots)
    chosen = jnp.argsort(scores, stable=True)[:NBLK].astype(jnp.int32)
    block_order = jax.random.permutation(keys[2], NBLK).astype(jnp.int32)
    return chosen[block_order]


def level_of(key, shape, cuts, low, top_value):
    def one(axis_at, shards_of):
        draws = jax.random.uniform(jax.random.fold_in(jax.random.fold_in(key, 6), axis_at), (shards_of,), jnp.float32, low / len(cuts), top_value / len(cuts))
        return jnp.repeat(jnp.exp(draws), shape[axis_at] // shards_of).reshape((-1,) + (1,) * (len(shape) - axis_at - 1))

    factor_of = one(*cuts[0])
    for cut in cuts[1:]:
        factor_of = factor_of * one(*cut)
    return factor_of


def noise(own_key, dims, deviation, bound, pieces=(), held_as=jnp.bfloat16):
    loudness = level_of(own_key, dims, pieces, -0.22, 0.18) if pieces else 1.0
    drawn = jax.random.normal(own_key, dims, jnp.float32) * deviation * loudness
    return jnp.minimum(jnp.maximum(drawn, -bound), bound).astype(held_as)


def setup_inputs(seed: int = 0) -> dict:
    streams_of = jax.random.split(jax.random.key(seed), 7)
    tokens = draw_tokens(jax.random.fold_in(streams_of[6], 71), 0)
    norm_gain = jnp.clip(1.0 + 0.18 * jax.random.normal(streams_of[1], (D,), jnp.float32), 0.1, 1.9)
    key_bias = noise(streams_of[2], (KVW,), 1.0, 4.0, (), jnp.float32)
    key_weight = noise(streams_of[3], (SLOTS * BLK, KVW), D ** -0.5, 0.078125, ((0, 16),))
    cotangent = draw_cotangent(jax.random.fold_in(streams_of[6], 71), 0)
    block_slot = draw_block_slot(jax.random.fold_in(streams_of[6], 71), 0)
    return dict(tokens=tokens, norm_gain=norm_gain, key_bias=key_bias, key_weight=key_weight, cotangent=cotangent, block_slot=block_slot)


EPS = 1e-06

def normalize(tokens, norm_gain):
    values = tokens.astype(jnp.float32)
    inv_rms = lax.rsqrt(lax.optimization_barrier(jnp.mean(values * values, axis=-1, keepdims=True)) + EPS)
    normed = (values * inv_rms * norm_gain).astype(jnp.bfloat16)
    return (values, inv_rms, normed)

def token_backward(values, inv_rms, grad_normed, norm_gain):
    scaled = grad_normed * norm_gain
    inner = lax.optimization_barrier(jnp.mean(scaled * values, axis=-1, keepdims=True))
    return (inv_rms * (scaled - values * inv_rms * inv_rms * inner)).astype(jnp.bfloat16)

def reference(tokens, norm_gain, key_bias, key_weight, cotangent, block_slot):
    whole_weight = key_weight.reshape(SLOTS, BLK, KVW)[block_slot.astype(jnp.int32)].reshape(D, KVW)
    grad_scale = float(ALL_TOK) ** (-0.5)
    device_count = ALL_TOK // TOK_DEV

    def per_device(totals, blocks):
        tok_rows, cot_rows = blocks
        values, inv_rms, normed = normalize(tok_rows, norm_gain)
        forward = jnp.dot(normed, whole_weight, preferred_element_type=jnp.float32)
        projected = (forward + key_bias).astype(jnp.bfloat16)
        grad_normed = lax.dot_general(cot_rows, whole_weight, (((1,), (1,)), ((), ())), preferred_element_type=jnp.float32)
        token_grad = token_backward(values, inv_rms, grad_normed, norm_gain)
        partial_grad = lax.dot_general(normed, cot_rows, (((0,), (0,)), ((), ())), preferred_element_type=jnp.float32) * grad_scale
        rounded = lax.optimization_barrier(partial_grad.astype(jnp.bfloat16)).astype(jnp.float32)
        gain_term = lax.optimization_barrier(jnp.sum(grad_normed * values * inv_rms, axis=0)) * grad_scale
        bias_term = lax.optimization_barrier(jnp.sum(cot_rows.astype(jnp.float32), axis=0)) * grad_scale
        return ((totals[0] + rounded, totals[1] + gain_term, totals[2] + bias_term), (projected, token_grad))
    start = (jnp.zeros((D, KVW), jnp.float32), jnp.zeros((D,), jnp.float32), jnp.zeros((KVW,), jnp.float32))
    totals, outputs = lax.scan(per_device, start, (tokens.reshape(device_count, TOK_DEV, D), cotangent.reshape(device_count, TOK_DEV, KVW)))
    weight_sum, gain_grad, bias_grad = totals
    projected = outputs[0].reshape(ALL_TOK, KVW)
    token_grad = outputs[1].reshape(ALL_TOK, D)
    weight_grad = jnp.zeros((SLOTS, BLK, KVW), jnp.float32).at[block_slot.astype(jnp.int32)].set(weight_sum.reshape(NBLK, BLK, KVW)).reshape(SLOTS * BLK, KVW)
    return (projected, token_grad, weight_grad, gain_grad, bias_grad)
```

```python
import jax
import jax.numpy as jnp
from jax import lax
from jax.experimental import pallas as pl
from jax.experimental.pallas import tpu as pltpu
from jax.sharding import PartitionSpec as P

BLK = 128
EPS = 1e-06
AXES = ("shard", "rep")
BF = jnp.bfloat16
F32 = jnp.float32


def _flat(x, y, z, c):
    return ((x // 2) * 8 + z * 2 + c) * 8 + (x % 2) * 4 + y


def _pairs(move):
    return [
        (_flat(x, y, z, c), _flat(*move(x, y, z, c)))
        for x in range(4)
        for y in range(4)
        for z in range(4)
        for c in range(2)
    ]


def _turn(axis, k, place):
    place = list(place)
    place[axis] = (place[axis] + k) % 4
    return tuple(place)


def _send(v, move):
    return lax.ppermute(v, AXES, _pairs(move))


def send_core(v):
    return _send(v, lambda x, y, z, c: (x, y, z, 1 - c))


X, Y, Z = 0, 1, 2
STAGE = {"a": (Y, Z), "b": (Z, Y)}
SHIFTS = (1, 3, 2)


def send_on(axes, v, k):
    return _send(v, lambda *p: _turn(axes[p[3]], k, p[:3]) + (p[3],))


def inv_rms_of(values):
    return lax.rsqrt(jnp.mean(values * values, axis=-1, keepdims=True) + EPS)


CHUNK = 1280
STRIP = 1280


def _cols(tile):
    return pl.ds(pl.multiple_of(tile * BLK, BLK), BLK)


def _terms_kernel(scale, tiles, inv, other_inv, cot, other_cot, own, other, gain, *rest):
    outs, pair = rest[:7], rest[7]
    rows, width = own.shape
    steps = width // STRIP
    for i in range(4):
        pair[:rows, i * BLK : (i + 1) * BLK] = cot[:, _cols(tiles[i])]
        pair[rows:, i * BLK : (i + 1) * BLK] = other_cot[:, _cols(tiles[i])]

    def body(at, own, other, gain, *parts):
        j = at.index[0]
        g = gain[...]
        one = (own[...].astype(F32) * inv[...] * g).astype(BF)
        two = (other[...].astype(F32) * other_inv[...] * g).astype(BF)
        terms = lax.dot_general(
            jnp.concatenate([one, two]),
            pair[...],
            (((0,), (0,)), ((), ())),
            preferred_element_type=F32,
        )
        terms = (terms * scale).astype(BF)
        parts[0][...] = terms[:, :BLK]

        @pl.when(j < steps // 2)
        def _():
            for i in range(1, 4):
                parts[2 * i - 1][...] = terms[:, i * BLK : (i + 1) * BLK]

        @pl.when(j >= steps // 2)
        def _():
            for i in range(1, 4):
                parts[2 * i][...] = terms[:, i * BLK : (i + 1) * BLK]

    strip = lambda j: (0, j)
    top = steps // 2
    upper = pl.BlockSpec((STRIP, BLK), lambda j: (jnp.minimum(j, top - 1), 0))
    lower = pl.BlockSpec((STRIP, BLK), lambda j: (jnp.maximum(j - top, 0), 0))
    pltpu.emit_pipeline(
        body,
        grid=(width // STRIP,),
        in_specs=[
            pl.BlockSpec((rows, STRIP), strip),
            pl.BlockSpec((rows, STRIP), strip),
            pl.BlockSpec((1, STRIP), strip),
        ],
        out_specs=[pl.BlockSpec((STRIP, BLK), lambda j: (j, 0))] + [upper, lower] * 3,
        _explicit_indices=True,
    )(own, other, gain, *outs)


def weight_terms(scale, tiles, own, other, inv, other_inv, gain, cot, other_cot):
    rows, width = own.shape
    vmem = pl.BlockSpec(memory_space=pltpu.VMEM)
    hbm = pl.BlockSpec(memory_space=pltpu.HBM)
    return pl.pallas_call(
        lambda *refs: _terms_kernel(scale, *refs),
        in_specs=[pl.BlockSpec(memory_space=pltpu.SMEM)] + [vmem] * 4 + [hbm] * 3,
        out_specs=[hbm] * 7,
        scratch_shapes=[pltpu.VMEM((2 * rows, 4 * BLK), BF)],
        out_shape=[jax.ShapeDtypeStruct((width, BLK), BF)]
        + [jax.ShapeDtypeStruct((width // 2, BLK), BF)] * 6,
        compiler_params=pltpu.CompilerParams(vmem_limit_bytes=56 * 1024 * 1024),
        name="weight_terms",
    )(tiles, inv, other_inv, cot, other_cot, own, other, gain)


def _tokens_kernel(tiles, tok, inv, gain, bias, cot, *rest):
    pieces, (proj, grad) = rest[:10], rest[10:12]
    turned, weight, acc, scaled, out, sems = rest[12:]
    _, width = tok.shape
    chunks = width // CHUNK
    for i in range(8):
        turned[:, i * BLK : (i + 1) * BLK] = cot[:, _cols(tiles[i])]
    r = inv[...]
    for j in range(chunks):
        at = slice(j * CHUNK, (j + 1) * CHUNK)
        for i in range(8):
            first = 5 * (i // 4) + i % 4
            piece, rows_at = pieces[first], at
            if i % 4 == 3 and j >= chunks // 2:
                half = chunks // 2 * CHUNK
                piece, rows_at = pieces[first + 1], slice(at.start - half, at.stop - half)
            weight[:, i * BLK : (i + 1) * BLK] = piece[rows_at]
        g = gain[:, at]
        normed = (tok[:, at].astype(F32) * r * g).astype(BF)
        part = jnp.dot(normed, weight[...], preferred_element_type=F32)
        if j == 0:
            acc[...] = part
        else:
            acc[...] += part
        grad_normed = lax.dot_general(
            turned[...], weight[...], (((1,), (1,)), ((), ())), preferred_element_type=F32
        )
        scaled[j] = grad_normed * g
    for i in range(8):
        cols = _cols(tiles[i])
        proj[:, cols] = (acc[:, i * BLK : (i + 1) * BLK] + bias[:, cols]).astype(BF)
    along = jnp.sum(acc[...] * turned[...].astype(F32), axis=1, keepdims=True)
    back = r * along * (1.0 / width)
    copies = []
    for j in range(chunks):
        at = slice(j * CHUNK, (j + 1) * CHUNK)
        out[j] = (r * (scaled[j] - tok[:, at].astype(F32) * back)).astype(BF)
        copies.append(pltpu.make_async_copy(out.at[j], grad.at[:, at], sems.at[j]))
        copies[-1].start()
    for copy in copies:
        copy.wait()


def token_work(tiles, tokens, inv, gain, bias, cot, pieces):
    rows, width = tokens.shape
    kvw = cot.shape[1]
    chunks = width // CHUNK
    vmem = pl.BlockSpec(memory_space=pltpu.VMEM)
    return pl.pallas_call(
        _tokens_kernel,
        in_specs=[pl.BlockSpec(memory_space=pltpu.SMEM)] + [vmem] * (5 + len(pieces)),
        out_specs=[vmem, pl.BlockSpec(memory_space=pltpu.HBM)],
        scratch_shapes=[
            pltpu.VMEM((rows, kvw), BF),
            pltpu.VMEM((CHUNK, kvw), BF),
            pltpu.VMEM((rows, kvw), F32),
            pltpu.VMEM((chunks, rows, CHUNK), F32),
            pltpu.VMEM((chunks, rows, CHUNK), BF),
            pltpu.SemaphoreType.DMA((chunks,)),
        ],
        out_shape=[
            jax.ShapeDtypeStruct((rows, kvw), BF),
            jax.ShapeDtypeStruct((rows, width), BF),
        ],
        compiler_params=pltpu.CompilerParams(vmem_limit_bytes=40 * 1024 * 1024),
        name="token_work",
    )(tiles, tokens, inv, gain, bias, cot, *pieces)


def small_kernel(body, outs, scalars, arrays, scratch=()):
    smem = pl.BlockSpec(memory_space=pltpu.SMEM)
    vmem = pl.BlockSpec(memory_space=pltpu.VMEM)
    return pl.pallas_call(
        body,
        in_specs=[smem] * len(scalars) + [vmem] * len(arrays),
        out_specs=[vmem] * len(outs),
        out_shape=[jax.ShapeDtypeStruct(*o) for o in outs],
        scratch_shapes=list(scratch),
    )(*scalars, *arrays)


def hi_lo(v):
    hi = v.astype(BF)
    return hi, (v - hi.astype(F32)).astype(BF)


def _place_kernel(index, one, two, three, four, out):
    for i, piece in enumerate((one, two, three, four)):
        out[:, index[i]] = piece[...]


def _merge_kernel(one, two, three, four, left, right):
    left[...] = (one[...].astype(F32) + two[...].astype(F32)).astype(BF)
    right[...] = (three[...].astype(F32) + four[...].astype(F32)).astype(BF)


def _split_kernel(index, own, top_1, top_2, bottom_1, bottom_2, *outs):
    half = top_1.shape[0]
    for i in range(4):
        at = index[i]
        total = own[:half, at].astype(F32) + top_1[:, at].astype(F32) + top_2[:, at].astype(F32)
        outs[i][:half] = total.astype(BF)
        total = own[half:, at].astype(F32) + bottom_1[:, at].astype(F32)
        outs[i][half:] = (total + bottom_2[:, at].astype(F32)).astype(BF)


def _owners_kernel(block_of_slot, row_block, one, two, three, four, w_rows, bias, out, blocks):
    nblk, rows, _ = one.shape
    total = one[...].astype(F32) + two[...].astype(F32)
    total += three[...].astype(F32) + four[...].astype(F32)
    blocks[:nblk] = total.astype(BF)
    blocks[nblk] = jnp.zeros((rows, BLK), BF)
    terms = jnp.sum(total * w_rows[...].astype(F32), axis=-1, keepdims=True)
    shape = (nblk, rows, BLK)
    lane = lax.broadcasted_iota(jnp.int32, shape, 2)
    row = lax.broadcasted_iota(jnp.int32, shape, 1)
    terms = jnp.where(lane == row + row_block[0] * rows, jnp.broadcast_to(terms, shape), 0.0)
    gain = jnp.sum(terms, axis=1).astype(BF)
    dests = out.shape[0]
    cap = block_of_slot.shape[0] // dests
    for dest in range(dests):
        for i in range(cap):
            out[dest, i * rows : (i + 1) * rows] = blocks[block_of_slot[dest * cap + i]]
        out[dest, cap * rows : cap * rows + nblk] = gain
        out[dest, cap * rows + nblk :] = bias[...]


def _pack(out, n, sums):
    hi, lo = hi_lo(sums)
    m = sums.shape[0]
    out[n : n + m] = hi
    out[n + m :] = lo


def _unpack(ref, n):
    m = (ref.shape[0] - n) // 2
    return ref[n : n + m].astype(F32) + ref[n + m :].astype(F32)


def _group_kernel(nblk, got, out):
    half = got.shape[0] // 2
    own = got.shape[1] - nblk - 16
    for i in range(half):
        pair = got[i, :own].astype(F32) + got[half + i, :own].astype(F32)
        out[i * own : (i + 1) * own] = pair.astype(BF)
    extra = jnp.sum(got[:, own:].astype(F32), axis=0)
    sums = jnp.concatenate([extra[:nblk], extra[nblk : nblk + 8] + extra[nblk + 8 :]])
    _pack(out, half * own, sums)


def _pair_kernel(n, one, two, out):
    out[:n] = (one[:n].astype(F32) + two[:n].astype(F32)).astype(BF)
    _pack(out, n, _unpack(one, n) + _unpack(two, n))


def _finish_kernel(n, cap, index, one, two, three, four, norm_gain, grad, gain, bias):
    sums = jnp.zeros((one.shape[0] - n, BLK), F32)[: (one.shape[0] - n) // 2]
    for i, piece in enumerate((one, two, three, four)):
        at = index[i]
        for z in range(4):
            for slot in range(cap):
                row = z * 2 * cap * 32 + slot * 32
                grad[slot * BLK + z * 32 : slot * BLK + z * 32 + 32, _cols(at)] = piece[
                    row : row + 32
                ].astype(F32)
                row += cap * 32
                rows = pl.ds(pl.multiple_of(slot * BLK + at * 32, 32), 32)
                grad[rows, (4 + z) * BLK : (5 + z) * BLK] = piece[row : row + 32].astype(F32)
        sums += _unpack(piece, n)
    nblk = norm_gain.shape[0]
    gain[...] = sums[:nblk] / norm_gain[...]
    bias[...] = sums[nblk:]


def local(tokens, norm_gain, key_bias, key_weight, cotangent, block_slot):
    rows, width = tokens.shape
    kvw = cotangent.shape[1]
    shards = lax.axis_size("shard")
    replicas = lax.axis_size("rep")
    cap = key_weight.shape[0] // BLK
    slots = shards * cap
    nblk = width // BLK
    grad_scale = float(rows * shards * replicas) ** (-0.5)
    s = lax.axis_index("shard")
    r = lax.axis_index("rep")
    core, z, xh = s & 1, (s >> 1) & 3, s >> 3
    xl, y = r >> 2, r & 3
    x = xh * 2 + xl
    place = (x, y, z)

    def along(axes, c=core):
        return jnp.where(c == 0, place[axes[0]], place[axes[1]])

    lag = jnp.array([0, 1, 3, 2], jnp.int32)
    me_a, me_b = (along(STAGE[stage]) for stage in "ab")
    order = jnp.concatenate(
        [4 * core + ((me_a - lag) & 3), 4 * (1 - core) + ((along(STAGE["a"], 1 - core) - lag) & 3)]
    )
    block_of_slot = (
        jnp.full((slots,), nblk, jnp.int32)
        .at[block_slot]
        .set(jnp.arange(nblk, dtype=jnp.int32))
    )

    other_tokens = send_core(tokens)
    other_cot = send_core(cotangent)
    inv_rms = inv_rms_of(tokens.astype(F32))
    other_inv = send_core(inv_rms)
    gain_row = norm_gain.reshape(1, width)
    terms = weight_terms(
        grad_scale,
        4 * core + ((me_a + lag) & 3),
        tokens,
        other_tokens,
        inv_rms,
        other_inv,
        gain_row,
        cotangent,
        other_cot,
    )
    bias_part = jnp.sum(cotangent.astype(F32), axis=0) * grad_scale
    bias_hi = lax.reduce_precision(bias_part, 8, 7)
    bias_rows = jnp.concatenate([bias_hi, bias_part - bias_hi]).astype(BF).reshape(16, BLK)
    four_parts = (nblk, 4, 32, BLK)
    own, top_1, bottom_1, top_3, bottom_3, top_2, bottom_2 = terms
    via_1 = send_on(STAGE["a"], top_2, 1)
    via_3 = send_on(STAGE["a"], bottom_2, 3)
    bottom_in = send_on(STAGE["a"], bottom_1, 1)
    top_in = send_on(STAGE["a"], top_3, 3)
    half_part = ((width // 2, BLK), BF)
    top_1, bottom_3 = small_kernel(
        _merge_kernel, [half_part] * 2, [], [top_1, via_1, bottom_3, via_3]
    )
    terms = [
        own, top_in, send_on(STAGE["a"], top_1, 1), bottom_in, send_on(STAGE["a"], bottom_3, 3)
    ]

    w_tiles = key_weight.reshape(cap, 4, 4, 8, 2, 4, BLK)

    def at(v, i, axis):
        return lax.dynamic_index_in_dim(v, i, axis=axis, keepdims=False)

    w_0 = at(w_tiles[:, :, :, :, 0], y, 4)
    w_1 = jnp.moveaxis(w_tiles[:, :, :, :, 1], 4, 0)
    halves = (2, 4, cap, 4, 8, BLK)
    pass_0 = jnp.moveaxis(at(w_0.reshape(cap, 2, 2, 4, 8, BLK), xl, 2), 1, 0)[:, None]
    pass_1 = jnp.moveaxis(at(w_1.reshape(4, cap, 2, 2, 4, 8, BLK), xl, 3), 2, 0)
    grad_0 = jnp.moveaxis(w_0, 1, 0)[None]
    grad_1 = at(w_1, y, 2)[None]
    to_shards = jnp.stack(
        [
            jnp.stack([jnp.broadcast_to(v, halves) for v in pair], axis=2)
            for pair in ((pass_0, pass_1), (grad_0, grad_1))
        ],
        axis=3,
    ).reshape(shards, 2 * cap * 4, 8, BLK)
    w_both = lax.all_to_all(to_shards, "shard", 0, 0, tiled=True)
    w_both = w_both.reshape(shards * 2 * cap, 32, BLK)
    at_slot = (block_slot >> 2) * (2 * cap) + (block_slot & 3)
    w_pass = [jnp.take(w_both, at_slot, axis=0, mode="clip")]
    w_rows = jnp.take(w_both, at_slot + cap, axis=0, mode="clip")
    w_pass += [send_on((X, X), w_pass[0], k) for k in SHIFTS]
    (w_b,) = small_kernel(_place_kernel, [(four_parts, BF)], [(x - lag) & 3], w_pass)
    w_b = w_b.reshape(width, BLK)
    w_own = [w_b] + [send_on(STAGE["a"], w_b, k) for k in (1, 3)]
    top = width // 2
    w_own.append(send_on(STAGE["a"], w_own[1][:top], 1))
    w_own.append(send_on(STAGE["a"], w_own[2][top:], 3))
    w_other = [send_core(p) for p in w_own]
    terms = small_kernel(
        _split_kernel,
        [((nblk, 32, BLK), BF)] * 4,
        [(me_b + lag) & 3],
        [t.reshape(-1, 4, 32, BLK) for t in terms],
    )
    terms = [terms[0]] + [send_on(STAGE["b"], terms[i + 1], k) for i, k in enumerate(SHIFTS)]

    projected, token_grad = token_work(
        order, tokens, inv_rms, gain_row, key_bias.reshape(1, kvw), cotangent, w_own + w_other
    )

    (to_owners,) = small_kernel(
        _owners_kernel,
        [((shards, cap * 32 + nblk + 16, BLK), BF)],
        [block_of_slot, me_b.reshape(1)],
        [*terms, w_rows, bias_rows],
        [pltpu.VMEM((nblk + 1, 32, BLK), BF)],
    )
    got = lax.all_to_all(to_owners, "shard", 0, 0, tiled=True)
    n_own = (shards // 2) * cap * 32
    message = ((n_own + 2 * (nblk + 8), BLK), BF)
    (mine,) = small_kernel(lambda *r: _group_kernel(nblk, *r), [message], [], [got])

    got = _send(mine, lambda x, y, z, c: (x ^ 1, y, z, c))
    (mine,) = small_kernel(lambda *r: _pair_kernel(n_own, *r), [message], [], [mine, got])
    got = [mine] + [send_on((Y, Y), mine, k) for k in SHIFTS]
    weight_grad, gain_grad, bias_grad = small_kernel(
        lambda *r: _finish_kernel(n_own, cap, *r),
        [((cap * BLK, kvw), F32), ((nblk, BLK), F32), ((8, BLK), F32)],
        [(y - lag) & 3],
        [*got, norm_gain.reshape(nblk, BLK)],
    )
    gain_grad = gain_grad.reshape(width)
    bias_grad = bias_grad.reshape(kvw)

    return (projected, token_grad, weight_grad, gain_grad, bias_grad)


def solution(mesh):
    return _mapped(mesh)


def _mapped(mesh):
    return jax.shard_map(
        local,
        mesh=mesh,
        in_specs=(
            P(("shard", "rep"), None),
            P(),
            P(),
            P("shard", None),
            P(("shard", "rep"), None),
            P(),
        ),
        out_specs=(
            P(("shard", "rep"), None),
            P(("shard", "rep"), None),
            P("shard", None),
            P(),
            P(),
        ),
        check_vma=False,
    )
```

```python
import jax
import jax.numpy as jnp
from jax import lax
from jax.experimental import pallas as pl
from jax.experimental.pallas import tpu as pltpu
from jax.sharding import PartitionSpec as P

BLK = 128
EPS = 1e-06
AXES = ("shard", "rep")
BF = jnp.bfloat16
F32 = jnp.float32


def _flat(x, y, z, c):
    return ((x // 2) * 8 + z * 2 + c) * 8 + (x % 2) * 4 + y


def _pairs(move):
    return [
        (_flat(x, y, z, c), _flat(*move(x, y, z, c)))
        for x in range(4)
        for y in range(4)
        for z in range(4)
        for c in range(2)
    ]


def _turn(axis, k, place):
    place = list(place)
    place[axis] = (place[axis] + k) % 4
    return tuple(place)


def _send(v, move):
    return lax.ppermute(v, AXES, _pairs(move))


def send_core(v):
    return _send(v, lambda x, y, z, c: (x, y, z, 1 - c))


X, Y, Z = 0, 1, 2
STAGE = {"a": (Y, Z), "b": (Z, Y)}
SHIFTS = (1, 3, 2)


def send_on(axes, v, k):
    return _send(v, lambda *p: _turn(axes[p[3]], k, p[:3]) + (p[3],))


def inv_rms_of(values):
    return lax.rsqrt(jnp.mean(values * values, axis=-1, keepdims=True) + EPS)


CHUNK = 1280
STRIP = 1280


def _cols(tile):
    return pl.ds(pl.multiple_of(tile * BLK, BLK), BLK)


def _terms_kernel(scale, tiles, inv, other_inv, cot, other_cot, own, other, gain, *rest):
    outs, pair = rest[:7], rest[7]
    rows, width = own.shape
    steps = width // STRIP
    for i in range(4):
        pair[:rows, i * BLK : (i + 1) * BLK] = cot[:, _cols(tiles[i])]
        pair[rows:, i * BLK : (i + 1) * BLK] = other_cot[:, _cols(tiles[i])]

    def body(at, own, other, gain, *parts):
        j = at.index[0]
        g = gain[...]
        one = (own[...].astype(F32) * inv[...] * g).astype(BF)
        two = (other[...].astype(F32) * other_inv[...] * g).astype(BF)
        terms = lax.dot_general(
            jnp.concatenate([one, two]),
            pair[...],
            (((0,), (0,)), ((), ())),
            preferred_element_type=F32,
        )
        terms = (terms * scale).astype(BF)
        parts[0][...] = terms[:, :BLK]

        @pl.when(j < steps // 2)
        def _():
            for i in range(1, 4):
                parts[2 * i - 1][...] = terms[:, i * BLK : (i + 1) * BLK]

        @pl.when(j >= steps // 2)
        def _():
            for i in range(1, 4):
                parts[2 * i][...] = terms[:, i * BLK : (i + 1) * BLK]

    strip = lambda j: (0, j)
    top = steps // 2
    upper = pl.BlockSpec((STRIP, BLK), lambda j: (jnp.minimum(j, top - 1), 0))
    lower = pl.BlockSpec((STRIP, BLK), lambda j: (jnp.maximum(j - top, 0), 0))
    pltpu.emit_pipeline(
        body,
        grid=(width // STRIP,),
        in_specs=[
            pl.BlockSpec((rows, STRIP), strip),
            pl.BlockSpec((rows, STRIP), strip),
            pl.BlockSpec((1, STRIP), strip),
        ],
        out_specs=[pl.BlockSpec((STRIP, BLK), lambda j: (j, 0))] + [upper, lower] * 3,
        _explicit_indices=True,
    )(own, other, gain, *outs)


def weight_terms(scale, tiles, own, other, inv, other_inv, gain, cot, other_cot):
    rows, width = own.shape
    vmem = pl.BlockSpec(memory_space=pltpu.VMEM)
    hbm = pl.BlockSpec(memory_space=pltpu.HBM)
    return pl.pallas_call(
        lambda *refs: _terms_kernel(scale, *refs),
        in_specs=[pl.BlockSpec(memory_space=pltpu.SMEM)] + [vmem] * 4 + [hbm] * 3,
        out_specs=[hbm] * 7,
        scratch_shapes=[pltpu.VMEM((2 * rows, 4 * BLK), BF)],
        out_shape=[jax.ShapeDtypeStruct((width, BLK), BF)]
        + [jax.ShapeDtypeStruct((width // 2, BLK), BF)] * 6,
        compiler_params=pltpu.CompilerParams(vmem_limit_bytes=56 * 1024 * 1024),
        name="weight_terms",
    )(tiles, inv, other_inv, cot, other_cot, own, other, gain)


def _tokens_kernel(tiles, tok, inv, gain, bias, cot, *rest):
    pieces, (proj, grad) = rest[:10], rest[10:12]
    turned, weight, acc, scaled, out, sems, loads = rest[12:]
    _, width = tok.shape
    chunks = width // CHUNK
    pulls = []
    for j in range(chunks):
        half = chunks // 2 * CHUNK
        for i in range(8):
            first = 5 * (i // 4) + i % 4
            lower = i % 4 == 3 and j >= chunks // 2
            start = j * CHUNK - (half if lower else 0)
            pulls.append(
                pltpu.make_async_copy(
                    pieces[first + lower].at[start : start + CHUNK],
                    weight.at[j, :, i * BLK : (i + 1) * BLK],
                    loads.at[j, i],
                )
            )
            pulls[-1].start()
    for i in range(8):
        turned[:, i * BLK : (i + 1) * BLK] = cot[:, _cols(tiles[i])]
    r = inv[...]
    for j in range(chunks):
        at = slice(j * CHUNK, (j + 1) * CHUNK)
        for pull in pulls[8 * j : 8 * j + 8]:
            pull.wait()
        g = gain[:, at]
        normed = (tok[:, at].astype(F32) * r * g).astype(BF)
        part = jnp.dot(normed, weight[j], preferred_element_type=F32)
        if j == 0:
            acc[...] = part
        else:
            acc[...] += part
        grad_normed = lax.dot_general(
            turned[...], weight[j], (((1,), (1,)), ((), ())), preferred_element_type=F32
        )
        scaled[j] = grad_normed * g
    for i in range(8):
        cols = _cols(tiles[i])
        proj[:, cols] = (acc[:, i * BLK : (i + 1) * BLK] + bias[:, cols]).astype(BF)
    along = jnp.sum(acc[...] * turned[...].astype(F32), axis=1, keepdims=True)
    back = r * along * (1.0 / width)
    copies = []
    for j in range(chunks):
        at = slice(j * CHUNK, (j + 1) * CHUNK)
        out[j] = (r * (scaled[j] - tok[:, at].astype(F32) * back)).astype(BF)
        copies.append(pltpu.make_async_copy(out.at[j], grad.at[:, at], sems.at[j]))
        copies[-1].start()
    for copy in copies:
        copy.wait()


def token_work(tiles, tokens, inv, gain, bias, cot, pieces):
    rows, width = tokens.shape
    kvw = cot.shape[1]
    chunks = width // CHUNK
    vmem = pl.BlockSpec(memory_space=pltpu.VMEM)
    return pl.pallas_call(
        _tokens_kernel,
        in_specs=[pl.BlockSpec(memory_space=pltpu.SMEM)]
        + [vmem] * 5
        + [pl.BlockSpec(memory_space=pltpu.HBM)] * len(pieces),
        out_specs=[vmem, pl.BlockSpec(memory_space=pltpu.HBM)],
        scratch_shapes=[
            pltpu.VMEM((rows, kvw), BF),
            pltpu.VMEM((chunks, CHUNK, kvw), BF),
            pltpu.VMEM((rows, kvw), F32),
            pltpu.VMEM((chunks, rows, CHUNK), F32),
            pltpu.VMEM((chunks, rows, CHUNK), BF),
            pltpu.SemaphoreType.DMA((chunks,)),
            pltpu.SemaphoreType.DMA((chunks, 8)),
        ],
        out_shape=[
            jax.ShapeDtypeStruct((rows, kvw), BF),
            jax.ShapeDtypeStruct((rows, width), BF),
        ],
        compiler_params=pltpu.CompilerParams(vmem_limit_bytes=40 * 1024 * 1024),
        name="token_work",
    )(tiles, tokens, inv, gain, bias, cot, *pieces)


def small_kernel(body, outs, scalars, arrays, scratch=()):
    smem = pl.BlockSpec(memory_space=pltpu.SMEM)
    vmem = pl.BlockSpec(memory_space=pltpu.VMEM)
    return pl.pallas_call(
        body,
        in_specs=[smem] * len(scalars) + [vmem] * len(arrays),
        out_specs=[vmem] * len(outs),
        out_shape=[jax.ShapeDtypeStruct(*o) for o in outs],
        scratch_shapes=list(scratch),
    )(*scalars, *arrays)


def hi_lo(v):
    hi = v.astype(BF)
    return hi, (v - hi.astype(F32)).astype(BF)


def _place_kernel(index, one, two, three, four, out):
    for i, piece in enumerate((one, two, three, four)):
        out[:, index[i]] = piece[...]


def _merge_kernel(one, two, three, four, left, right):
    left[...] = (one[...].astype(F32) + two[...].astype(F32)).astype(BF)
    right[...] = (three[...].astype(F32) + four[...].astype(F32)).astype(BF)


def _split_kernel(index, own, top_1, top_2, bottom_1, bottom_2, *outs):
    half = top_1.shape[0]
    for i in range(4):
        at = index[i]
        total = own[:half, at].astype(F32) + top_1[:, at].astype(F32) + top_2[:, at].astype(F32)
        outs[i][:half] = total.astype(BF)
        total = own[half:, at].astype(F32) + bottom_1[:, at].astype(F32)
        outs[i][half:] = (total + bottom_2[:, at].astype(F32)).astype(BF)


def _owners_kernel(block_of_slot, row_block, one, two, three, four, w_rows, bias, out, blocks):
    nblk, rows, _ = one.shape
    total = one[...].astype(F32) + two[...].astype(F32)
    total += three[...].astype(F32) + four[...].astype(F32)
    blocks[:nblk] = total.astype(BF)
    blocks[nblk] = jnp.zeros((rows, BLK), BF)
    terms = jnp.sum(total * w_rows[...].astype(F32), axis=-1, keepdims=True)
    shape = (nblk, rows, BLK)
    lane = lax.broadcasted_iota(jnp.int32, shape, 2)
    row = lax.broadcasted_iota(jnp.int32, shape, 1)
    terms = jnp.where(lane == row + row_block[0] * rows, jnp.broadcast_to(terms, shape), 0.0)
    gain = jnp.sum(terms, axis=1).astype(BF)
    dests = out.shape[0]
    cap = block_of_slot.shape[0] // dests
    for dest in range(dests):
        for i in range(cap):
            out[dest, i * rows : (i + 1) * rows] = blocks[block_of_slot[dest * cap + i]]
        out[dest, cap * rows : cap * rows + nblk] = gain
        out[dest, cap * rows + nblk :] = bias[...]


def _pack(out, n, sums):
    hi, lo = hi_lo(sums)
    m = sums.shape[0]
    out[n : n + m] = hi
    out[n + m :] = lo


def _unpack(ref, n):
    m = (ref.shape[0] - n) // 2
    return ref[n : n + m].astype(F32) + ref[n + m :].astype(F32)


def _group_kernel(nblk, got, out):
    half = got.shape[0] // 2
    own = got.shape[1] - nblk - 16
    for i in range(half):
        pair = got[i, :own].astype(F32) + got[half + i, :own].astype(F32)
        out[i * own : (i + 1) * own] = pair.astype(BF)
    extra = jnp.sum(got[:, own:].astype(F32), axis=0)
    sums = jnp.concatenate([extra[:nblk], extra[nblk : nblk + 8] + extra[nblk + 8 :]])
    _pack(out, half * own, sums)


def _pair_kernel(n, one, two, out):
    out[:n] = (one[:n].astype(F32) + two[:n].astype(F32)).astype(BF)
    _pack(out, n, _unpack(one, n) + _unpack(two, n))


def _finish_kernel(n, cap, index, one, two, three, four, norm_gain, grad, gain, bias):
    sums = jnp.zeros((one.shape[0] - n, BLK), F32)[: (one.shape[0] - n) // 2]
    for i, piece in enumerate((one, two, three, four)):
        at = index[i]
        for z in range(4):
            for slot in range(cap):
                row = z * 2 * cap * 32 + slot * 32
                grad[slot * BLK + z * 32 : slot * BLK + z * 32 + 32, _cols(at)] = piece[
                    row : row + 32
                ].astype(F32)
                row += cap * 32
                rows = pl.ds(pl.multiple_of(slot * BLK + at * 32, 32), 32)
                grad[rows, (4 + z) * BLK : (5 + z) * BLK] = piece[row : row + 32].astype(F32)
        sums += _unpack(piece, n)
    nblk = norm_gain.shape[0]
    gain[...] = sums[:nblk] / norm_gain[...]
    bias[...] = sums[nblk:]


def local(tokens, norm_gain, key_bias, key_weight, cotangent, block_slot):
    rows, width = tokens.shape
    kvw = cotangent.shape[1]
    shards = lax.axis_size("shard")
    replicas = lax.axis_size("rep")
    cap = key_weight.shape[0] // BLK
    slots = shards * cap
    nblk = width // BLK
    grad_scale = float(rows * shards * replicas) ** (-0.5)
    s = lax.axis_index("shard")
    r = lax.axis_index("rep")
    core, z, xh = s & 1, (s >> 1) & 3, s >> 3
    xl, y = r >> 2, r & 3
    x = xh * 2 + xl
    place = (x, y, z)

    def along(axes, c=core):
        return jnp.where(c == 0, place[axes[0]], place[axes[1]])

    lag = jnp.array([0, 1, 3, 2], jnp.int32)
    me_a, me_b = (along(STAGE[stage]) for stage in "ab")
    order = jnp.concatenate(
        [4 * core + ((me_a - lag) & 3), 4 * (1 - core) + ((along(STAGE["a"], 1 - core) - lag) & 3)]
    )
    block_of_slot = (
        jnp.full((slots,), nblk, jnp.int32)
        .at[block_slot]
        .set(jnp.arange(nblk, dtype=jnp.int32))
    )

    other_tokens = send_core(tokens)
    other_cot = send_core(cotangent)
    inv_rms = inv_rms_of(tokens.astype(F32))
    other_inv = send_core(inv_rms)
    gain_row = norm_gain.reshape(1, width)
    terms = weight_terms(
        grad_scale,
        4 * core + ((me_a + lag) & 3),
        tokens,
        other_tokens,
        inv_rms,
        other_inv,
        gain_row,
        cotangent,
        other_cot,
    )
    bias_part = jnp.sum(cotangent.astype(F32), axis=0) * grad_scale
    bias_hi = lax.reduce_precision(bias_part, 8, 7)
    bias_rows = jnp.concatenate([bias_hi, bias_part - bias_hi]).astype(BF).reshape(16, BLK)
    four_parts = (nblk, 4, 32, BLK)
    own, top_1, bottom_1, top_3, bottom_3, top_2, bottom_2 = terms
    via_1 = send_on(STAGE["a"], top_2, 1)
    via_3 = send_on(STAGE["a"], bottom_2, 3)
    bottom_in = send_on(STAGE["a"], bottom_1, 1)
    top_in = send_on(STAGE["a"], top_3, 3)
    half_part = ((width // 2, BLK), BF)
    top_1, bottom_3 = small_kernel(
        _merge_kernel, [half_part] * 2, [], [top_1, via_1, bottom_3, via_3]
    )
    terms = [
        own, top_in, send_on(STAGE["a"], top_1, 1), bottom_in, send_on(STAGE["a"], bottom_3, 3)
    ]

    w_tiles = key_weight.reshape(cap, 4, 4, 8, 2, 4, BLK)

    def at(v, i, axis):
        return lax.dynamic_index_in_dim(v, i, axis=axis, keepdims=False)

    w_0 = at(w_tiles[:, :, :, :, 0], y, 4)
    w_1 = jnp.moveaxis(w_tiles[:, :, :, :, 1], 4, 0)
    halves = (2, 4, cap, 4, 8, BLK)
    pass_0 = jnp.moveaxis(at(w_0.reshape(cap, 2, 2, 4, 8, BLK), xl, 2), 1, 0)[:, None]
    pass_1 = jnp.moveaxis(at(w_1.reshape(4, cap, 2, 2, 4, 8, BLK), xl, 3), 2, 0)
    grad_0 = jnp.moveaxis(w_0, 1, 0)[None]
    grad_1 = at(w_1, y, 2)[None]
    to_shards = jnp.stack(
        [
            jnp.stack([jnp.broadcast_to(v, halves) for v in pair], axis=2)
            for pair in ((pass_0, pass_1), (grad_0, grad_1))
        ],
        axis=3,
    ).reshape(shards, 2 * cap * 4, 8, BLK)
    w_both = lax.all_to_all(to_shards, "shard", 0, 0, tiled=True)
    w_both = w_both.reshape(shards * 2 * cap, 32, BLK)
    at_slot = (block_slot >> 2) * (2 * cap) + (block_slot & 3)
    w_pass = [jnp.take(w_both, at_slot, axis=0, mode="clip")]
    w_rows = jnp.take(w_both, at_slot + cap, axis=0, mode="clip")
    w_pass += [send_on((X, X), w_pass[0], k) for k in SHIFTS]
    (w_b,) = small_kernel(_place_kernel, [(four_parts, BF)], [(x - lag) & 3], w_pass)
    w_b = w_b.reshape(width, BLK)
    w_own = [w_b] + [send_on(STAGE["a"], w_b, k) for k in (1, 3)]
    top = width // 2
    w_own.append(send_on(STAGE["a"], w_own[1][:top], 1))
    w_own.append(send_on(STAGE["a"], w_own[2][top:], 3))
    w_other = [send_core(p) for p in w_own]
    terms = small_kernel(
        _split_kernel,
        [((nblk, 32, BLK), BF)] * 4,
        [(me_b + lag) & 3],
        [t.reshape(-1, 4, 32, BLK) for t in terms],
    )
    terms = [terms[0]] + [send_on(STAGE["b"], terms[i + 1], k) for i, k in enumerate(SHIFTS)]

    projected, token_grad = token_work(
        order, tokens, inv_rms, gain_row, key_bias.reshape(1, kvw), cotangent, w_own + w_other
    )

    (to_owners,) = small_kernel(
        _owners_kernel,
        [((shards, cap * 32 + nblk + 16, BLK), BF)],
        [block_of_slot, me_b.reshape(1)],
        [*terms, w_rows, bias_rows],
        [pltpu.VMEM((nblk + 1, 32, BLK), BF)],
    )
    got = lax.all_to_all(to_owners, "shard", 0, 0, tiled=True)
    n_own = (shards // 2) * cap * 32
    message = ((n_own + 2 * (nblk + 8), BLK), BF)
    (mine,) = small_kernel(lambda *r: _group_kernel(nblk, *r), [message], [], [got])

    got = _send(mine, lambda x, y, z, c: (x ^ 1, y, z, c))
    (mine,) = small_kernel(lambda *r: _pair_kernel(n_own, *r), [message], [], [mine, got])
    got = [mine] + [send_on((Y, Y), mine, k) for k in SHIFTS]
    weight_grad, gain_grad, bias_grad = small_kernel(
        lambda *r: _finish_kernel(n_own, cap, *r),
        [((cap * BLK, kvw), F32), ((nblk, BLK), F32), ((8, BLK), F32)],
        [(y - lag) & 3],
        [*got, norm_gain.reshape(nblk, BLK)],
    )
    gain_grad = gain_grad.reshape(width)
    bias_grad = bias_grad.reshape(kvw)

    return (projected, token_grad, weight_grad, gain_grad, bias_grad)


def solution(mesh):
    return _mapped(mesh)


def _mapped(mesh):
    return jax.shard_map(
        local,
        mesh=mesh,
        in_specs=(
            P(("shard", "rep"), None),
            P(),
            P(),
            P("shard", None),
            P(("shard", "rep"), None),
            P(),
        ),
        out_specs=(
            P(("shard", "rep"), None),
            P(("shard", "rep"), None),
            P("shard", None),
            P(),
            P(),
        ),
        check_vma=False,
    )
```
